32 devices in a mesh: row: 8 (over z, x), col: 4 (over y, core).
Axes of the slice: x: 2, y: 2, z: 4, core: 2. Of those that a mesh axis runs over, the one named last changes fastest.
Arguments:
- old_params: float32 [2, 64, 131072], P(None, ('row', 'col')), may hold values from -0.12 to 0.12
- old_first: float32 [2, 64, 131072], P(None, ('row', 'col')), may hold values from -1.8 to 1.8
- old_second: float32 [2, 64, 131072], P(None, ('row', 'col')), may hold values from 0.001 to 1
- gradients: float32 [2, 32, 262144], P(None, ('row', 'col')), may hold values from -250 to 250
- old_table: int32 [2, 64], replicated, may hold values from 0 to 63, as said below
- new_table: int32 [2, 32], replicated, may hold values from 0 to 31, as said below
Outputs:
- new_params: float32 [2, 32, 262144], P(None, ('row', 'col'))
- new_first: float32 [2, 32, 262144], P(None, ('row', 'col'))
- new_second: float32 [2, 32, 262144], P(None, ('row', 'col'))
The draws below stay inside these ranges and needn't reach their ends.
Inputs may be any that keep to these rules, and one draw needn't show every extreme that they name: old_table[t, p] = p XOR k for one k per tensor. new_table[t, q] = q XOR k for one k per tensor.
All inputs are finite; a program needn't handle non-finite values.
Results may differ from the reference program's by a relative error of at most 0.00002.
Values sent between devices are 32-bit elements; how exact they have to be, the bound alone decides.
A program may use at most 64 MiB of HBM per device.

```python
import math
import jax
import jax.numpy as jnp

STEP = 100
NT = 2
ELEMS = 8388608
OLD_SHARDS = 64
OB = 131072
DEVICES = 32


def draw_old_table(key, part):
    folded = jax.random.fold_in(key, 11)
    offsets = jax.random.randint(folded, (NT, 1), 0, OLD_SHARDS)
    return jnp.bitwise_xor(jnp.arange(OLD_SHARDS, dtype=jnp.int32)[None, :], offsets).astype(jnp.int32)


def draw_new_table(key, part):
    folded = jax.random.fold_in(key, 23)
    offsets = jax.random.randint(folded, (NT, 1), 0, DEVICES)
    return jnp.bitwise_xor(jnp.arange(DEVICES, dtype=jnp.int32)[None, :], offsets).astype(jnp.int32)


def draw_gradients(key, part):
    folded = jax.random.fold_in(key, 37)
    key_private = jax.random.fold_in(folded, 0)
    position = jnp.arange(DEVICES, dtype=jnp.float32)[None, :, None]
    rising = 1.0 + 2.0 * position / max(DEVICES - 1, 1)
    private = jnp.clip(jax.random.normal(key_private, (NT, DEVICES, 2 * OB)), -8.0, 8.0)
    return (rising * private).astype(jnp.float32)


def shard_levels(own_key, shape, cuts, smallest, top_value):
    factor_of, own = 1.0, jax.random.fold_in(own_key, 6)
    for axis_at, parts in cuts:
        draws = jnp.exp(jax.random.uniform(jax.random.fold_in(own, axis_at), (parts,), jnp.float32, smallest / len(cuts), top_value / len(cuts)))
        factor_of = factor_of * jnp.repeat(draws, shape[axis_at] // parts).reshape([-1 if axis == axis_at else 1 for axis in range(len(shape))])
    return factor_of


def noise(key, shape, spread, most, cuts=(), held_as=jnp.bfloat16):
    gain = shard_levels(key, shape, cuts, -0.22, 0.18) if cuts else 1.0
    entries = jax.random.normal(key, shape, jnp.float32) * spread * gain
    return jnp.minimum(jnp.maximum(entries, -most), most).astype(held_as)


def setup_inputs(seed: int = 0) -> dict:
    seeds = jax.random.split(jax.random.key(seed), 7)
    return {
        "old_params": noise(seeds[0], (NT, OLD_SHARDS, OB), 0.02, 0.12, ((1, 32),), jnp.float32),
        "old_first": noise(seeds[1], (NT, OLD_SHARDS, OB), 0.3, 1.8, ((1, 32),), jnp.float32),
        "old_second": jnp.clip(jnp.exp(math.log(1.0) - 6.9077552 * jax.random.uniform(seeds[2], (NT, OLD_SHARDS, OB), jnp.float32) ** shard_levels(seeds[2], (NT, OLD_SHARDS, OB), ((1, 32),), -0.2, 0.2)), 0.001, 1.0),
        "gradients": draw_gradients(jax.random.fold_in(seeds[6], 71), 0),
        "old_table": draw_old_table(jax.random.fold_in(seeds[6], 71), 0),
        "new_table": draw_new_table(jax.random.fold_in(seeds[6], 71), 0),
    }


beta_one = 0.9
beta_two = 0.95
epsilon = 1e-08
learn_rate = 0.001
decay_rate = 0.1

def relayout(old_state, old_table, new_table):
    tensors = jnp.arange(old_state.shape[0], dtype=jnp.int32)[:, None]
    blocks = jnp.zeros_like(old_state).at[tensors, old_table].set(old_state)
    paired = blocks.reshape(old_state.shape[0], old_state.shape[1] // 2, 2 * old_state.shape[2])
    return paired[tensors, new_table]

def adam_update(params, first_moment, second_moment, gradients, clip_factor):
    scaled = clip_factor * gradients
    first_new = beta_one * first_moment + (1.0 - beta_one) * scaled
    second_new = beta_two * second_moment + (1.0 - beta_two) * scaled * scaled
    bias_first = 1.0 - beta_one ** STEP
    bias_second = 1.0 - beta_two ** STEP
    update = first_new / bias_first / (jnp.sqrt(second_new / bias_second) + epsilon)
    params_new = params - learn_rate * (update + decay_rate * params)
    return (params_new, first_new, second_new)

def reference(old_params, old_first, old_second, gradients, old_table, new_table):
    moved_params = relayout(old_params, old_table, new_table)
    moved_first = relayout(old_first, old_table, new_table)
    moved_second = relayout(old_second, old_table, new_table)
    grad_norm = jnp.sqrt(jnp.sum(gradients * gradients))
    limit = jnp.float32(0.5 * (NT * ELEMS) ** 0.5)
    clip_factor = limit / jnp.maximum(grad_norm, limit)
    return adam_update(moved_params, moved_first, moved_second, gradients, clip_factor)
```

```python
import functools
import math

import jax
import jax.numpy as jnp
from jax import lax
from jax.experimental import pallas as pl
from jax.experimental.pallas import tpu as pltpu
from jax.sharding import PartitionSpec as P

STEP = 100
LANES = 128
AXES = ("row", "col")
JOINT_DEVICES = 32
CHUNKS = 4
MESH = pl.DeviceIdType.MESH


beta_one = 0.9
beta_two = 0.95
epsilon = 1e-08
learn_rate = 0.001
decay_rate = 0.1


def adam_update(params, first_moment, second_moment, gradients, clip_factor):
    scaled = clip_factor * gradients
    first_new = beta_one * first_moment + (1.0 - beta_one) * scaled
    second_new = beta_two * second_moment + (1.0 - beta_two) * scaled * scaled
    bias_first = 1.0 - beta_one**STEP
    bias_second = 1.0 - beta_two**STEP
    update = first_new / bias_first / (jnp.sqrt(second_new / bias_second) + epsilon)
    params_new = params - learn_rate * (update + decay_rate * params)
    return (params_new, first_new, second_new)


def partner(key):
    columns = lax.axis_size(AXES[1])
    return (
        jnp.bitwise_xor(lax.axis_index(AXES[0]), key // columns),
        jnp.bitwise_xor(lax.axis_index(AXES[1]), key % columns),
    )


def squares_kernel(devices, grad_ref, out_ref, total, parts, send_sems, recv_sems):
    barrier = pltpu.get_barrier_semaphore()
    for key in range(1, devices):
        pl.semaphore_signal(barrier, inc=1, device_id=partner(key), device_id_type=MESH)
    grads = grad_ref[...]
    parts[0] = jnp.sum((grads * grads).reshape(-1, 8, LANES), axis=0)
    pl.semaphore_wait(barrier, devices - 1)
    copies = [
        pltpu.make_async_remote_copy(
            src_ref=parts.at[0],
            dst_ref=parts.at[key],
            send_sem=send_sems.at[key],
            recv_sem=recv_sems.at[key],
            device_id=partner(key),
            device_id_type=MESH,
        )
        for key in range(1, devices)
    ]
    for copy in copies:
        copy.start()
    for copy in copies:
        copy.wait()
    out_ref[...] = jnp.sum(parts[...], axis=0)


def sum_squares(gradients, devices):
    flat = gradients.reshape(-1, LANES)
    return pl.pallas_call(
        functools.partial(squares_kernel, devices),
        in_specs=[pl.BlockSpec(memory_space=pltpu.VMEM)],
        out_specs=pl.BlockSpec(memory_space=pltpu.VMEM),
        out_shape=jax.ShapeDtypeStruct((8, LANES), jnp.float32),
        scratch_shapes=[
            pltpu.VMEM((8, LANES), jnp.float32),
            pltpu.VMEM((devices, 8, LANES), jnp.float32),
            pltpu.SemaphoreType.DMA((devices,)),
            pltpu.SemaphoreType.DMA((devices,)),
        ],
        compiler_params=pltpu.CompilerParams(collective_id=0, has_side_effects=True),
        name="sum_squares",
    )(flat)


def move_kernel(jobs, params_ref, first_ref, second_ref, out_ref, recv_sems, send_sem, pass_sem, passed_sem):
    states = (params_ref, first_ref, second_ref)
    moves = [(slot, tensor, key) for slot, (tensor, key) in enumerate(jobs) if key]
    stays = [(slot, tensor) for slot, (tensor, key) in enumerate(jobs) if not key]
    peers = sorted({1} | {key for _, _, key in moves})
    places = {key: partner(key) for key in peers}
    barrier = pltpu.get_barrier_semaphore()
    for place in places.values():
        pl.semaphore_signal(barrier, inc=1, device_id=place, device_id_type=MESH)
    pl.semaphore_wait(barrier, len(peers))
    chunks = recv_sems.shape[1]
    halves = params_ref.shape[2]
    rows = params_ref.shape[1] // chunks

    def span(chunk):
        return pl.ds(pl.multiple_of(chunk * rows, rows), rows)

    def pick(turn):
        (slot, tensor, key), (other_slot, other_tensor, other_key) = moves[0], moves[-1]
        if len(moves) == 1:
            return slot, tensor, places[key]
        place = places[key]
        if key != other_key:
            place = tuple(jnp.where(turn == 0, a, b) for a, b in zip(place, places[other_key]))
        return turn, turn, place

    def across(source, slot, window):
        return pltpu.make_async_remote_copy(
            src_ref=source,
            dst_ref=out_ref.at[(1, slot, *window)],
            send_sem=pass_sem,
            recv_sem=passed_sem,
            device_id=places[1],
            device_id_type=MESH,
        )

    def start(step, _):
        slot, tensor, place = pick(lax.rem(step, len(moves)))
        piece = lax.div(step, len(moves))
        chunk, half = lax.div(piece, halves), lax.rem(piece, halves)
        for number, state in enumerate(states):
            pltpu.make_async_remote_copy(
                src_ref=state.at[tensor, span(chunk), half, 0],
                dst_ref=out_ref.at[0, slot, number, half, span(chunk)],
                send_sem=send_sem,
                recv_sem=recv_sems.at[slot, chunk],
                device_id=place,
                device_id_type=MESH,
            ).start()
        return 0

    def relay(step, _):
        slot, _, place = pick(lax.rem(step, len(moves)))
        chunk = lax.div(step, len(moves))
        landed = out_ref.at[0, slot, :, :, span(chunk)]
        pltpu.make_async_copy(landed, landed, recv_sems.at[slot, chunk]).wait()
        across(landed, slot, (slice(None), slice(None), span(chunk))).start()
        return 0

    if moves:
        lax.fori_loop(0, chunks * halves * len(moves), start, 0)
    for slot, tensor in stays:
        for number, state in enumerate(states):
            for half in range(halves):
                source = state.at[tensor, :, half, 0]
                across(source, slot, (number, half)).start()
                pltpu.make_async_copy(source, out_ref.at[0, slot, number, half], recv_sems.at[slot, 0]).start()
    if moves:
        lax.fori_loop(0, chunks * len(moves), relay, 0)
        sent = out_ref.at[0, pl.ds(0, len(moves))]
        pltpu.make_async_copy(sent, sent, send_sem).wait()
    for slot, _ in stays:
        kept = out_ref.at[0, slot]
        pltpu.make_async_copy(kept, kept, recv_sems.at[slot, 0]).wait()
    passed = out_ref.at[1]
    pltpu.make_async_copy(passed, passed, pass_sem).wait()
    pltpu.make_async_copy(passed, passed, passed_sem).wait()


def move(jobs, number, arrays):
    _, rows, halves, _, lanes = arrays[0].shape
    chunks = min(CHUNKS, rows)
    return pl.pallas_call(
        functools.partial(move_kernel, jobs),
        in_specs=[pl.BlockSpec(memory_space=pl.ANY)] * 3,
        out_specs=pl.BlockSpec(memory_space=pl.ANY),
        out_shape=jax.ShapeDtypeStruct((2, len(jobs), 3, halves, rows, lanes), jnp.float32),
        scratch_shapes=[pltpu.SemaphoreType.DMA((len(jobs), chunks))] + [pltpu.SemaphoreType.DMA] * 3,
        compiler_params=pltpu.CompilerParams(collective_id=number, has_side_effects=True),
        name="move_" + "_".join(str(key) for _, key in jobs),
    )(*arrays)


def update_kernel(table_ref, clip_ref, moved_ref, grad_ref, params_out, first_out, second_out):
    params, first, second = adam_update(
        moved_ref[0, 0, 0, 0], moved_ref[0, 0, 1, 0], moved_ref[0, 0, 2, 0], grad_ref[0, 0], clip_ref[0]
    )
    params_out[0, 0] = params
    first_out[0, 0] = first
    second_out[0, 0] = second


def update(table, clip_factor, moved, gradients):
    tensors, halves, rows, lanes = gradients.shape
    step = min(rows, 256)
    flat_spec = pl.BlockSpec((1, 1, step, lanes), lambda t, h, i, table: (t, h, i, 0))
    moved_spec = pl.BlockSpec(
        (1, 1, 3, 1, step, lanes), lambda t, h, i, table: (table[0, t], t, 0, jnp.bitwise_xor(h, table[1, t]), i, 0)
    )
    return pl.pallas_call(
        update_kernel,
        grid_spec=pltpu.PrefetchScalarGridSpec(
            num_scalar_prefetch=1,
            grid=(tensors, halves, rows // step),
            in_specs=[pl.BlockSpec(memory_space=pltpu.SMEM), moved_spec, flat_spec],
            out_specs=[flat_spec] * 3,
        ),
        out_shape=[jax.ShapeDtypeStruct(gradients.shape, jnp.float32)] * 3,
        name="update",
    )(table, clip_factor, moved, gradients)


def shards(old_params, old_first, old_second, gradients, old_table, new_table):
    tensors, halves, width = old_params.shape
    devices = lax.axis_size(AXES)
    rows = width // LANES
    old_key = old_table[:, 0]
    keys = jnp.bitwise_xor(jnp.right_shift(old_key, 1), new_table[:, 0])
    table = jnp.stack([jnp.bitwise_and(keys, 1), jnp.bitwise_and(old_key, 1)])
    chip_keys = jnp.right_shift(keys, 1)

    def paired(array):
        return array.reshape(tensors, halves, rows, 1, LANES).transpose(0, 2, 1, 3, 4)

    flat = gradients.reshape(tensors, halves, rows, LANES)
    total_squares = jnp.sum(sum_squares(gradients, devices))
    limit = jnp.float32(0.5 * math.sqrt(gradients.size * devices))
    clip_factor = limit / jnp.maximum(jnp.sqrt(total_squares), limit)
    chips = devices // 2
    states = (paired(old_params), paired(old_first), paired(old_second))
    if devices <= JOINT_DEVICES:
        pairs = [(2 * (i // chips), 2 * (i % chips)) for i in range(chips * chips)]
        branches = [functools.partial(move, tuple(enumerate(pair)), 1 + i) for i, pair in enumerate(pairs)]
        moved = lax.switch(chip_keys[0] * chips + chip_keys[1], branches, states)
    else:
        moved = []
        for tensor in range(tensors):
            branches = [
                functools.partial(move, ((tensor, 2 * i),), 1 + tensor * chips + i) for i in range(chips)
            ]
            moved.append(lax.switch(chip_keys[tensor], branches, states))
        moved = jnp.concatenate(moved, axis=1)
    results = update(table, clip_factor.reshape(1), moved, flat)
    return tuple(result.reshape(gradients.shape) for result in results)


def solution(mesh):
    spec = P(None, AXES, None)
    return jax.shard_map(
        shards,
        mesh=mesh,
        in_specs=(spec, spec, spec, spec, P(), P()),
        out_specs=(spec, spec, spec),
        check_vma=False,
    )
```

```python
import functools
import math

import jax
import jax.numpy as jnp
from jax import lax
from jax.experimental import pallas as pl
from jax.experimental.pallas import tpu as pltpu
from jax.sharding import PartitionSpec as P

STEP = 100
LANES = 128
AXES = ("row", "col")
JOINT_DEVICES = 32
GROUPS = 4
SPLIT = 4
PART = 256
BLOCK = 64
MESH = pl.DeviceIdType.MESH


beta_one = 0.9
beta_two = 0.95
epsilon = 1e-08
learn_rate = 0.001
decay_rate = 0.1


def adam_update(params, first_moment, second_moment, gradients, clip_factor):
    scaled = clip_factor * gradients
    first_new = beta_one * first_moment + (1.0 - beta_one) * scaled
    second_new = beta_two * second_moment + (1.0 - beta_two) * scaled * scaled
    rate = learn_rate / (1.0 - beta_one**STEP)
    unbias = 1.0 / (1.0 - beta_two**STEP)
    update = first_new * rate / (jnp.sqrt(second_new * unbias) + epsilon)
    params_new = params * (1.0 - learn_rate * decay_rate) - update
    return (params_new, first_new, second_new)


def partner(key):
    columns = lax.axis_size(AXES[1])
    return (
        jnp.bitwise_xor(lax.axis_index(AXES[0]), key // columns),
        jnp.bitwise_xor(lax.axis_index(AXES[1]), key % columns),
    )


def move_kernel(jobs, params_ref, first_ref, second_ref, out_ref, landed_sems, sent_sem, passed_sem):
    states = (params_ref, first_ref, second_ref)
    moves = [(slot, tensor, key) for slot, (tensor, key) in enumerate(jobs) if key]
    stays = [(slot, tensor) for slot, (tensor, key) in enumerate(jobs) if not key]
    peers = sorted({1} | {key for _, _, key in moves})
    places = {key: partner(key) for key in peers}
    barrier = pltpu.get_barrier_semaphore()
    for place in places.values():
        pl.semaphore_signal(barrier, inc=1, device_id=place, device_id_type=MESH)
    pl.semaphore_wait(barrier, len(peers))
    (groups,) = landed_sems.shape
    halves = params_ref.shape[2]
    group_rows = params_ref.shape[1] // groups
    rows = max(group_rows // SPLIT, 1)
    split = group_rows // rows

    def span(start, size):
        return pl.ds(pl.multiple_of(start * size, size), size)

    def turn(step):
        (slot, tensor, key), (_, _, other) = moves[0], moves[-1]
        if len(moves) == 1:
            return slot, tensor, places[key], step
        bit = jnp.bitwise_and(step, 1)
        place = places[key]
        if key != other:
            place = tuple(jnp.where(bit == 0, a, b) for a, b in zip(place, places[other]))
        return bit, bit, place, jnp.right_shift(step, 1)

    def window(slot, tensor, piece):
        half, chunk = jnp.bitwise_and(piece, 1), jnp.right_shift(piece, 1)
        for number, state in enumerate(states):
            source = state.at[tensor, span(chunk, rows), half, 0]
            yield source, out_ref.at[0, slot, number, half, span(chunk, rows)], landed_sems.at[lax.div(chunk, split)]

    def start(step, _):
        slot, tensor, place, piece = turn(step)
        for source, target, landed_sem in window(slot, tensor, piece):
            pltpu.make_async_remote_copy(
                src_ref=source,
                dst_ref=target,
                send_sem=sent_sem,
                recv_sem=landed_sem,
                device_id=place,
                device_id_type=MESH,
            ).start()
        return 0

    def keep(step, _):
        slot, tensor, piece = stays[0] + (step,)
        if len(stays) == 2:
            slot, piece = jnp.bitwise_and(step, 1), jnp.right_shift(step, 1)
            tensor = slot
        for source, target, landed_sem in window(slot, tensor, piece):
            pltpu.make_async_copy(source, target, landed_sem).start()
        return 0

    def relay(group, _):
        landed = out_ref.at[0, :, :, :, span(group, group_rows)]
        pltpu.make_async_copy(landed, landed, landed_sems.at[group]).wait()
        pltpu.make_async_remote_copy(
            src_ref=landed,
            dst_ref=out_ref.at[1, :, :, :, span(group, group_rows)],
            send_sem=sent_sem,
            recv_sem=passed_sem,
            device_id=places[1],
            device_id_type=MESH,
        ).start()
        return 0

    pieces = groups * split * halves
    if moves:
        lax.fori_loop(0, pieces * len(moves), start, 0)
    if stays:
        lax.fori_loop(0, pieces * len(stays), keep, 0)
    lax.fori_loop(0, groups, relay, 0)
    passed = out_ref.at[1]
    sent = passed if stays else out_ref
    pltpu.make_async_copy(sent, sent, sent_sem).wait()
    if moves and stays:
        moved = out_ref.at[0, moves[0][0]]
        pltpu.make_async_copy(moved, moved, sent_sem).wait()
    pltpu.make_async_copy(passed, passed, passed_sem).wait()


def move(jobs, number, arrays):
    _, rows, halves, _, lanes = arrays[0].shape
    groups = min(GROUPS, rows)
    return pl.pallas_call(
        functools.partial(move_kernel, jobs),
        in_specs=[pl.BlockSpec(memory_space=pl.ANY)] * 3,
        out_specs=pl.BlockSpec(memory_space=pl.ANY),
        out_shape=jax.ShapeDtypeStruct((2, len(jobs), 3, halves, rows, lanes), jnp.float32),
        scratch_shapes=[pltpu.SemaphoreType.DMA((groups,))] + [pltpu.SemaphoreType.DMA] * 2,
        compiler_params=pltpu.CompilerParams(
            collective_id=number, has_side_effects=True, vmem_limit_bytes=1 << 20
        ),
        name="move_" + "_".join(str(key) for _, key in jobs),
    )(*arrays)


def update_kernel(table_ref, clip_ref, moved_ref, grad_ref, params_out, first_out, second_out, *scratch):
    moved, grads, results, moved_sems, grad_sems, out_sems = scratch
    parts, _, rows, _ = moved.shape
    halves = grad_ref.shape[1]
    blocks = grad_ref.shape[2] // rows
    block_rows = min(rows, BLOCK)
    outs = (params_out, first_out, second_out)
    clip_factor = clip_ref[0]

    def place(part):
        block, shard = lax.rem(part, blocks), lax.div(part, blocks)
        return lax.div(shard, halves), lax.rem(shard, halves), pl.ds(pl.multiple_of(block * rows, rows), rows)

    def loads(part):
        tensor, half, span = place(part)
        source = moved_ref.at[table_ref[0, tensor], tensor, :, jnp.bitwise_xor(half, table_ref[1, tensor]), span]
        return (
            pltpu.make_async_copy(source, moved.at[part], moved_sems.at[part]),
            pltpu.make_async_copy(grad_ref.at[tensor, half, span], grads.at[part], grad_sems.at[part]),
        )

    def stores(part):
        tensor, half, span = place(part)
        return [
            pltpu.make_async_copy(results.at[part, number], out.at[tensor, half, span], out_sems.at[number, part])
            for number, out in enumerate(outs)
        ]

    def load(part, _):
        for copy in loads(part):
            copy.start()
        return 0

    def compute(part, _):
        for copy in loads(part):
            copy.wait()

        def block(number, _):
            span = pl.ds(pl.multiple_of(number * block_rows, block_rows), block_rows)
            values = adam_update(
                moved[part, 0, span], moved[part, 1, span], moved[part, 2, span], grads[part, span], clip_factor
            )
            for number, value in enumerate(values):
                results[part, number, span] = value
            return 0

        lax.fori_loop(0, rows // block_rows, block, 0)
        for copy in stores(part):
            copy.start()
        return 0

    def finish(part, _):
        for copy in stores(part):
            copy.wait()
        return 0

    lax.fori_loop(0, parts, load, 0)
    lax.fori_loop(0, parts, compute, 0)
    lax.fori_loop(0, parts, finish, 0)


def update(table, clip_factor, moved, gradients):
    tensors, halves, rows, lanes = gradients.shape
    step = min(rows, PART)
    parts = tensors * halves * (rows // step)
    return pl.pallas_call(
        update_kernel,
        in_specs=[pl.BlockSpec(memory_space=pltpu.SMEM)] * 2 + [pl.BlockSpec(memory_space=pl.ANY)] * 2,
        out_specs=[pl.BlockSpec(memory_space=pl.ANY)] * 3,
        out_shape=[jax.ShapeDtypeStruct(gradients.shape, jnp.float32)] * 3,
        scratch_shapes=[
            pltpu.VMEM((parts, 3, step, lanes), jnp.float32),
            pltpu.VMEM((parts, step, lanes), jnp.float32),
            pltpu.VMEM((parts, 3, step, lanes), jnp.float32),
            pltpu.SemaphoreType.DMA((parts,)),
            pltpu.SemaphoreType.DMA((parts,)),
            pltpu.SemaphoreType.DMA((3, parts)),
        ],
        compiler_params=pltpu.CompilerParams(vmem_limit_bytes=16 << 20),
        name="update",
    )(table, clip_factor, moved, gradients)


def shards(old_params, old_first, old_second, gradients, old_table, new_table):
    tensors, halves, width = old_params.shape
    devices = lax.axis_size(AXES)
    rows = width // LANES
    old_key = old_table[:, 0]
    keys = jnp.bitwise_xor(jnp.right_shift(old_key, 1), new_table[:, 0])
    table = jnp.stack([jnp.bitwise_and(keys, 1), jnp.bitwise_and(old_key, 1)])
    chip_keys = jnp.right_shift(keys, 1)

    def paired(array):
        return array.reshape(tensors, halves, rows, 1, LANES).transpose(0, 2, 1, 3, 4)

    flat = gradients.reshape(tensors, halves, rows, LANES)
    local_squares = jnp.sum(gradients * gradients)
    squares = lax.all_to_all(jnp.broadcast_to(local_squares, (devices, LANES)), AXES, 0, 0, tiled=True)
    total_squares = jnp.sum(squares[:, 0])
    limit = jnp.float32(0.5 * math.sqrt(gradients.size * devices))
    clip_factor = limit / jnp.maximum(jnp.sqrt(total_squares), limit)
    chips = devices // 2
    states = (paired(old_params), paired(old_first), paired(old_second))
    if devices <= JOINT_DEVICES:

        def inner(one, arrays):
            branches = [
                functools.partial(move, ((0, 2 * one), (1, 2 * two)), one * chips + two) for two in range(chips)
            ]
            return lax.switch(chip_keys[1], branches, arrays)

        moved = lax.switch(chip_keys[0], [functools.partial(inner, one) for one in range(chips)], states)
    else:
        moved = []
        for tensor in range(tensors):
            branches = [
                functools.partial(move, ((tensor, 2 * i),), tensor * chips + i) for i in range(chips)
            ]
            moved.append(lax.switch(chip_keys[tensor], branches, states))
        moved = jnp.concatenate(moved, axis=1)
    results = update(table, clip_factor.reshape(1), moved, flat)
    return tuple(result.reshape(gradients.shape) for result in results)


def solution(mesh):
    spec = P(None, AXES, None)
    return jax.shard_map(
        shards,
        mesh=mesh,
        in_specs=(spec, spec, spec, spec, P(), P()),
        out_specs=(spec, spec, spec),
        check_vma=False,
    )
```

```python
import functools
import math

import jax
import jax.numpy as jnp
from jax import lax
from jax.experimental import pallas as pl
from jax.experimental.pallas import tpu as pltpu
from jax.sharding import PartitionSpec as P

STEP = 100
LANES = 128
AXES = ("row", "col")
JOINT_DEVICES = 32
GROUPS = 4
SPLIT = 4
PART = 256
BLOCK = 64
SUM_ROWS = 256
MESH = pl.DeviceIdType.MESH


beta_one = 0.9
beta_two = 0.95
epsilon = 1e-08
learn_rate = 0.001
decay_rate = 0.1


def adam_update(params, first_moment, second_moment, gradients, clip_factor):
    scaled = clip_factor * gradients
    first_new = beta_one * first_moment + (1.0 - beta_one) * scaled
    second_new = beta_two * second_moment + (1.0 - beta_two) * scaled * scaled
    rate = learn_rate / (1.0 - beta_one**STEP)
    unbias = 1.0 / (1.0 - beta_two**STEP)
    update = first_new * rate / (jnp.sqrt(second_new * unbias) + epsilon)
    params_new = params * (1.0 - learn_rate * decay_rate) - update
    return (params_new, first_new, second_new)


def partner(key):
    columns = lax.axis_size(AXES[1])
    return (
        jnp.bitwise_xor(lax.axis_index(AXES[0]), key // columns),
        jnp.bitwise_xor(lax.axis_index(AXES[1]), key % columns),
    )


def clip_kernel(devices, limit, grad_ref, clip_ref, parts, sent_sem, landed_sem):
    barrier = pltpu.get_barrier_semaphore()

    def greet(key, _):
        pl.semaphore_signal(barrier, inc=1, device_id=partner(key), device_id_type=MESH)
        return 0

    lax.fori_loop(1, devices, greet, 0)
    lines = grad_ref.shape[0]
    step = min(lines, SUM_ROWS)

    def add(number, total):
        block = grad_ref[pl.ds(pl.multiple_of(number * step, step), step)]
        return total + jnp.sum((block * block).reshape(-1, 8, LANES), axis=0)

    squares = lax.fori_loop(0, lines // step, add, jnp.zeros((8, LANES), jnp.float32))
    parts[0] = jnp.sum(squares, axis=0, keepdims=True)
    pl.semaphore_wait(barrier, devices - 1)

    def send(key, _):
        pltpu.make_async_remote_copy(
            src_ref=parts.at[0],
            dst_ref=parts.at[key],
            send_sem=sent_sem,
            recv_sem=landed_sem,
            device_id=partner(key),
            device_id_type=MESH,
        ).start()
        return 0

    lax.fori_loop(1, devices, send, 0)
    others = parts.at[pl.ds(1, devices - 1)]
    pltpu.make_async_copy(others, others, landed_sem).wait()
    pltpu.make_async_copy(others, others, sent_sem).wait()
    total = jnp.sum(jnp.sum(parts[...], axis=0), axis=1, keepdims=True)
    clip_ref[...] = jnp.broadcast_to(limit / jnp.maximum(jnp.sqrt(total), limit), clip_ref.shape)


def clip_of(gradients, devices, number):
    limit = 0.5 * math.sqrt(gradients.size * devices)
    return pl.pallas_call(
        functools.partial(clip_kernel, devices, limit),
        in_specs=[pl.BlockSpec(memory_space=pltpu.VMEM)],
        out_specs=pl.BlockSpec(memory_space=pltpu.VMEM),
        out_shape=jax.ShapeDtypeStruct((1, LANES), jnp.float32),
        scratch_shapes=[
            pltpu.VMEM((devices, 1, LANES), jnp.float32),
            pltpu.SemaphoreType.DMA,
            pltpu.SemaphoreType.DMA,
        ],
        compiler_params=pltpu.CompilerParams(
            collective_id=number, has_side_effects=True, vmem_limit_bytes=4 << 20
        ),
        name="clip",
    )(gradients.reshape(-1, LANES))


def move_kernel(jobs, params_ref, first_ref, second_ref, out_ref, landed_sems, sent_sem, passed_sem):
    states = (params_ref, first_ref, second_ref)
    moves = [(slot, tensor, key) for slot, (tensor, key) in enumerate(jobs) if key]
    stays = [(slot, tensor) for slot, (tensor, key) in enumerate(jobs) if not key]
    peers = sorted({1} | {key for _, _, key in moves})
    places = {key: partner(key) for key in peers}
    barrier = pltpu.get_barrier_semaphore()
    for place in places.values():
        pl.semaphore_signal(barrier, inc=1, device_id=place, device_id_type=MESH)
    pl.semaphore_wait(barrier, len(peers))
    (groups,) = landed_sems.shape
    halves = params_ref.shape[2]
    group_rows = params_ref.shape[1] // groups
    rows = max(group_rows // SPLIT, 1)
    split = group_rows // rows

    def span(start, size):
        return pl.ds(pl.multiple_of(start * size, size), size)

    def turn(step):
        (slot, tensor, key), (_, _, other) = moves[0], moves[-1]
        if len(moves) == 1:
            return slot, tensor, places[key], step
        bit = jnp.bitwise_and(step, 1)
        place = places[key]
        if key != other:
            place = tuple(jnp.where(bit == 0, a, b) for a, b in zip(place, places[other]))
        return bit, bit, place, jnp.right_shift(step, 1)

    def window(slot, tensor, piece):
        half, chunk = jnp.bitwise_and(piece, 1), jnp.right_shift(piece, 1)
        for number, state in enumerate(states):
            source = state.at[tensor, span(chunk, rows), half, 0]
            yield source, out_ref.at[0, slot, number, half, span(chunk, rows)], landed_sems.at[lax.div(chunk, split)]

    def start(step, _):
        slot, tensor, place, piece = turn(step)
        for source, target, landed_sem in window(slot, tensor, piece):
            pltpu.make_async_remote_copy(
                src_ref=source,
                dst_ref=target,
                send_sem=sent_sem,
                recv_sem=landed_sem,
                device_id=place,
                device_id_type=MESH,
            ).start()
        return 0

    def keep(step, _):
        slot, tensor, piece = stays[0] + (step,)
        if len(stays) == 2:
            slot, piece = jnp.bitwise_and(step, 1), jnp.right_shift(step, 1)
            tensor = slot
        for source, target, landed_sem in window(slot, tensor, piece):
            pltpu.make_async_copy(source, target, landed_sem).start()
        return 0

    def relay(group, _):
        landed = out_ref.at[0, :, :, :, span(group, group_rows)]
        pltpu.make_async_copy(landed, landed, landed_sems.at[group]).wait()
        pltpu.make_async_remote_copy(
            src_ref=landed,
            dst_ref=out_ref.at[1, :, :, :, span(group, group_rows)],
            send_sem=sent_sem,
            recv_sem=passed_sem,
            device_id=places[1],
            device_id_type=MESH,
        ).start()
        return 0

    pieces = groups * split * halves
    if moves:
        lax.fori_loop(0, pieces * len(moves), start, 0)
    if stays:
        lax.fori_loop(0, pieces * len(stays), keep, 0)
    lax.fori_loop(0, groups, relay, 0)
    passed = out_ref.at[1]
    sent = passed if stays else out_ref
    pltpu.make_async_copy(sent, sent, sent_sem).wait()
    if moves and stays:
        moved = out_ref.at[0, moves[0][0]]
        pltpu.make_async_copy(moved, moved, sent_sem).wait()
    pltpu.make_async_copy(passed, passed, passed_sem).wait()


def move(jobs, number, arrays):
    _, rows, halves, _, lanes = arrays[0].shape
    groups = min(GROUPS, rows)
    return pl.pallas_call(
        functools.partial(move_kernel, jobs),
        in_specs=[pl.BlockSpec(memory_space=pl.ANY)] * 3,
        out_specs=pl.BlockSpec(memory_space=pl.ANY),
        out_shape=jax.ShapeDtypeStruct((2, len(jobs), 3, halves, rows, lanes), jnp.float32),
        scratch_shapes=[pltpu.SemaphoreType.DMA((groups,))] + [pltpu.SemaphoreType.DMA] * 2,
        compiler_params=pltpu.CompilerParams(
            collective_id=number, has_side_effects=True, vmem_limit_bytes=1 << 20
        ),
        name="move_" + "_".join(str(key) for _, key in jobs),
    )(*arrays)


def update_kernel(table_ref, clip_ref, moved_ref, grad_ref, params_out, first_out, second_out, *scratch):
    moved, results, moved_sems, out_sems = scratch
    parts, _, rows, _ = moved.shape
    halves = grad_ref.shape[1]
    blocks = grad_ref.shape[2] // rows
    block_rows = min(rows, BLOCK)
    outs = (params_out, first_out, second_out)
    clip_factor = clip_ref[...]

    def place(part):
        block, shard = lax.rem(part, blocks), lax.div(part, blocks)
        return lax.div(shard, halves), lax.rem(shard, halves), pl.ds(pl.multiple_of(block * rows, rows), rows)

    def load(part):
        tensor, half, span = place(part)
        source = moved_ref.at[table_ref[0, tensor], tensor, :, jnp.bitwise_xor(half, table_ref[1, tensor]), span]
        return pltpu.make_async_copy(source, moved.at[part], moved_sems.at[part])

    def stores(part):
        tensor, half, span = place(part)
        return [
            pltpu.make_async_copy(results.at[part, number], out.at[tensor, half, span], out_sems.at[number, part])
            for number, out in enumerate(outs)
        ]

    def begin(part, _):
        load(part).start()
        return 0

    def compute(part, _):
        load(part).wait()
        tensor, half, whole = place(part)

        def block(number, _):
            span = pl.ds(pl.multiple_of(number * block_rows, block_rows), block_rows)
            grads = grad_ref[tensor, half, pl.ds(pl.multiple_of(whole.start + number * block_rows, block_rows), block_rows)]
            values = adam_update(moved[part, 0, span], moved[part, 1, span], moved[part, 2, span], grads, clip_factor)
            for number, value in enumerate(values):
                results[part, number, span] = value
            return 0

        lax.fori_loop(0, rows // block_rows, block, 0)
        for copy in stores(part):
            copy.start()
        return 0

    def finish(part, _):
        for copy in stores(part):
            copy.wait()
        return 0

    lax.fori_loop(0, parts, begin, 0)
    lax.fori_loop(0, parts, compute, 0)
    lax.fori_loop(0, parts, finish, 0)


def update(table, clip_factor, moved, gradients):
    tensors, halves, rows, lanes = gradients.shape
    step = min(rows, PART)
    parts = tensors * halves * (rows // step)
    return pl.pallas_call(
        update_kernel,
        in_specs=[
            pl.BlockSpec(memory_space=pltpu.SMEM),
            pl.BlockSpec(memory_space=pltpu.VMEM),
            pl.BlockSpec(memory_space=pl.ANY),
            pl.BlockSpec(memory_space=pltpu.VMEM),
        ],
        out_specs=[pl.BlockSpec(memory_space=pl.ANY)] * 3,
        out_shape=[jax.ShapeDtypeStruct(gradients.shape, jnp.float32)] * 3,
        scratch_shapes=[
            pltpu.VMEM((parts, 3, step, lanes), jnp.float32),
            pltpu.VMEM((parts, 3, step, lanes), jnp.float32),
            pltpu.SemaphoreType.DMA((parts,)),
            pltpu.SemaphoreType.DMA((3, parts)),
        ],
        compiler_params=pltpu.CompilerParams(vmem_limit_bytes=20 << 20),
        name="update",
    )(table, clip_factor, moved, gradients)


def shards(old_params, old_first, old_second, gradients, old_table, new_table):
    tensors, halves, width = old_params.shape
    devices = lax.axis_size(AXES)
    rows = width // LANES
    old_key = old_table[:, 0]
    keys = jnp.bitwise_xor(jnp.right_shift(old_key, 1), new_table[:, 0])
    table = jnp.stack([jnp.bitwise_and(keys, 1), jnp.bitwise_and(old_key, 1)])
    chip_keys = jnp.right_shift(keys, 1)

    def paired(array):
        return array.reshape(tensors, halves, rows, 1, LANES).transpose(0, 2, 1, 3, 4)

    flat = gradients.reshape(tensors, halves, rows, LANES)
    clip_factor = clip_of(gradients, devices, 0)
    chip_keys, clip_factor = lax.optimization_barrier((chip_keys, clip_factor))
    chips = devices // 2
    states = (paired(old_params), paired(old_first), paired(old_second))
    if devices <= JOINT_DEVICES:

        def inner(one, arrays):
            branches = [
                functools.partial(move, ((0, 2 * one), (1, 2 * two)), 1 + one * chips + two) for two in range(chips)
            ]
            return lax.switch(chip_keys[1], branches, arrays)

        moved = lax.switch(chip_keys[0], [functools.partial(inner, one) for one in range(chips)], states)
    else:
        moved = []
        for tensor in range(tensors):
            branches = [
                functools.partial(move, ((tensor, 2 * i),), 1 + tensor * chips + i) for i in range(chips)
            ]
            moved.append(lax.switch(chip_keys[tensor], branches, states))
        moved = jnp.concatenate(moved, axis=1)
    results = update(table, clip_factor, moved, flat)
    return tuple(result.reshape(gradients.shape) for result in results)


def solution(mesh):
    spec = P(None, AXES, None)
    return jax.shard_map(
        shards,
        mesh=mesh,
        in_specs=(spec, spec, spec, spec, P(), P()),
        out_specs=(spec, spec, spec),
        check_vma=False,
    )
```

```python
import functools
import math

import jax
import jax.numpy as jnp
from jax import lax
from jax.experimental import pallas as pl
from jax.experimental.pallas import tpu as pltpu
from jax.sharding import PartitionSpec as P

STEP = 100
LANES = 128
AXES = ("row", "col")
JOINT_DEVICES = 32
GROUPS = 8
SPLIT = 2
PART = 256
BLOCK = 64
SUM_ROWS = 256
LOGICAL = pl.DeviceIdType.LOGICAL


beta_one = 0.9
beta_two = 0.95
epsilon = 1e-08
learn_rate = 0.001
decay_rate = 0.1


def adam_update(params, first_moment, second_moment, gradients, clip_factor):
    scaled = clip_factor * gradients
    first_new = beta_one * first_moment + (1.0 - beta_one) * scaled
    second_new = beta_two * second_moment + (1.0 - beta_two) * scaled * scaled
    rate = learn_rate / (1.0 - beta_one**STEP)
    unbias = 1.0 / (1.0 - beta_two**STEP)
    update = first_new * rate / (jnp.sqrt(second_new * unbias) + epsilon)
    params_new = params * (1.0 - learn_rate * decay_rate) - update
    return (params_new, first_new, second_new)


def partner(key):
    return jnp.bitwise_xor(lax.axis_index(AXES), key)


def clip_kernel(devices, limit, grad_ref, clip_ref, grads, parts, load_sems, sent_sem, landed_sem):
    step = grads.shape[1]
    loads = [
        pltpu.make_async_copy(grad_ref.at[pl.ds(number * step, step)], grads.at[number], load_sems.at[number])
        for number in range(grads.shape[0])
    ]
    for load in loads:
        load.start()
    barrier = pltpu.get_barrier_semaphore()

    def greet(step, _):
        pl.semaphore_signal(barrier, inc=1, device_id=partner(devices - step), device_id_type=LOGICAL)
        return 0

    lax.fori_loop(1, devices, greet, 0)
    rows = min(step, SUM_ROWS)
    squares = jnp.zeros((8, LANES), jnp.float32)
    for number, load in enumerate(loads):
        load.wait()

        def add(line, total, number=number):
            block = grads[number, pl.ds(pl.multiple_of(line * rows, rows), rows)]
            return total + jnp.sum((block * block).reshape(-1, 8, LANES), axis=0)

        squares = lax.fori_loop(0, step // rows, add, squares)
    parts[0] = jnp.sum(squares, axis=0, keepdims=True)
    pl.semaphore_wait(barrier, devices - 1)

    def send(step, _):
        key = devices - step
        pltpu.make_async_remote_copy(
            src_ref=parts.at[0],
            dst_ref=parts.at[key],
            send_sem=sent_sem,
            recv_sem=landed_sem,
            device_id=partner(key),
            device_id_type=LOGICAL,
        ).start()
        return 0

    lax.fori_loop(1, devices, send, 0)
    others = parts.at[pl.ds(1, devices - 1)]
    pltpu.make_async_copy(others, others, landed_sem).wait()
    pltpu.make_async_copy(others, others, sent_sem).wait()
    total = jnp.sum(jnp.sum(parts[...], axis=0), axis=1, keepdims=True)
    clip_ref[...] = jnp.broadcast_to(limit / jnp.maximum(jnp.sqrt(total), limit), clip_ref.shape)


def clip_of(gradients, devices, number):
    limit = 0.5 * math.sqrt(gradients.size * devices)
    loads = 2
    step = gradients.size // LANES // loads
    return pl.pallas_call(
        functools.partial(clip_kernel, devices, limit),
        in_specs=[pl.BlockSpec(memory_space=pl.ANY)],
        out_specs=pl.BlockSpec(memory_space=pltpu.VMEM),
        out_shape=jax.ShapeDtypeStruct((1, LANES), jnp.float32),
        scratch_shapes=[
            pltpu.VMEM((loads, step, LANES), jnp.float32),
            pltpu.VMEM((devices, 1, LANES), jnp.float32),
            pltpu.SemaphoreType.DMA((loads,)),
            pltpu.SemaphoreType.DMA,
            pltpu.SemaphoreType.DMA,
        ],
        compiler_params=pltpu.CompilerParams(collective_id=number, has_side_effects=True),
        name="clip",
    )(gradients.reshape(-1, LANES))


def move_kernel(jobs, params_ref, first_ref, second_ref, out_ref, landed_sems, sent_sem, passed_sem):
    states = (params_ref, first_ref, second_ref)
    moves = [(slot, tensor, key) for slot, (tensor, key) in enumerate(jobs) if key]
    stays = [(slot, tensor) for slot, (tensor, key) in enumerate(jobs) if not key]
    peers = sorted({1} | {key for _, _, key in moves})
    places = {key: partner(key) for key in peers}
    barrier = pltpu.get_barrier_semaphore()
    for place in places.values():
        pl.semaphore_signal(barrier, inc=1, device_id=place, device_id_type=LOGICAL)
    pl.semaphore_wait(barrier, len(peers))
    (groups,) = landed_sems.shape
    halves = params_ref.shape[2]
    group_rows = params_ref.shape[1] // groups
    rows = max(group_rows // SPLIT, 1)
    split = group_rows // rows

    def span(start, size):
        return pl.ds(pl.multiple_of(start * size, size), size)

    def turn(step):
        (slot, tensor, key), (_, _, other) = moves[0], moves[-1]
        if len(moves) == 1:
            return slot, tensor, places[key], step
        bit = jnp.bitwise_and(step, 1)
        place = places[key]
        if key != other:
            place = jnp.where(bit == 0, place, places[other])
        return bit, bit, place, jnp.right_shift(step, 1)

    def window(slot, tensor, piece):
        half, chunk = jnp.bitwise_and(piece, 1), jnp.right_shift(piece, 1)
        for number, state in enumerate(states):
            source = state.at[tensor, span(chunk, rows), half, 0]
            yield source, out_ref.at[0, slot, number, half, span(chunk, rows)], landed_sems.at[lax.div(chunk, split)]

    def start(step, _):
        slot, tensor, place, piece = turn(step)
        for source, target, landed_sem in window(slot, tensor, piece):
            pltpu.make_async_remote_copy(
                src_ref=source,
                dst_ref=target,
                send_sem=sent_sem,
                recv_sem=landed_sem,
                device_id=place,
                device_id_type=LOGICAL,
            ).start()
        return 0

    def keep(step, _):
        slot, tensor, piece = stays[0] + (step,)
        if len(stays) == 2:
            slot, piece = jnp.bitwise_and(step, 1), jnp.right_shift(step, 1)
            tensor = slot
        for source, target, landed_sem in window(slot, tensor, piece):
            pltpu.make_async_copy(source, target, landed_sem).start()
        return 0

    def relay(group, _):
        landed = out_ref.at[0, :, :, :, span(group, group_rows)]
        pltpu.make_async_copy(landed, landed, landed_sems.at[group]).wait()
        pltpu.make_async_remote_copy(
            src_ref=landed,
            dst_ref=out_ref.at[1, :, :, :, span(group, group_rows)],
            send_sem=sent_sem,
            recv_sem=passed_sem,
            device_id=places[1],
            device_id_type=LOGICAL,
        ).start()
        return 0

    pieces = groups * split * halves
    if moves:
        lax.fori_loop(0, pieces * len(moves), start, 0)
    if stays:
        lax.fori_loop(0, pieces * len(stays), keep, 0)
    lax.fori_loop(0, groups, relay, 0)
    passed = out_ref.at[1]
    sent = passed if stays else out_ref
    pltpu.make_async_copy(sent, sent, sent_sem).wait()
    if moves and stays:
        moved = out_ref.at[0, moves[0][0]]
        pltpu.make_async_copy(moved, moved, sent_sem).wait()
    pltpu.make_async_copy(passed, passed, passed_sem).wait()


def move(jobs, number, arrays):
    _, rows, halves, _, lanes = arrays[0].shape
    groups = min(GROUPS, rows)
    return pl.pallas_call(
        functools.partial(move_kernel, jobs),
        in_specs=[pl.BlockSpec(memory_space=pl.ANY)] * 3,
        out_specs=pl.BlockSpec(memory_space=pl.ANY),
        out_shape=jax.ShapeDtypeStruct((2, len(jobs), 3, halves, rows, lanes), jnp.float32),
        scratch_shapes=[pltpu.SemaphoreType.DMA((groups,))] + [pltpu.SemaphoreType.DMA] * 2,
        compiler_params=pltpu.CompilerParams(
            collective_id=number, has_side_effects=True, vmem_limit_bytes=1 << 20
        ),
        name="move_" + "_".join(str(key) for _, key in jobs),
    )(*arrays)


def update_kernel(table_ref, clip_ref, moved_ref, grad_ref, params_out, first_out, second_out, *scratch):
    moved, results, moved_sems, out_sems = scratch
    parts, _, rows, _ = moved.shape
    halves = grad_ref.shape[1]
    blocks = grad_ref.shape[2] // rows
    block_rows = min(rows, BLOCK)
    outs = (params_out, first_out, second_out)
    clip_factor = clip_ref[...]

    def place(part):
        block, shard = lax.rem(part, blocks), lax.div(part, blocks)
        return lax.div(shard, halves), lax.rem(shard, halves), pl.ds(pl.multiple_of(block * rows, rows), rows)

    def load(part):
        tensor, half, span = place(part)
        source = moved_ref.at[table_ref[0, tensor], tensor, :, jnp.bitwise_xor(half, table_ref[1, tensor]), span]
        return pltpu.make_async_copy(source, moved.at[part], moved_sems.at[part])

    def stores(part):
        tensor, half, span = place(part)
        return [
            pltpu.make_async_copy(results.at[part, number], out.at[tensor, half, span], out_sems.at[number, part])
            for number, out in enumerate(outs)
        ]

    def begin(part, _):
        load(part).start()
        return 0

    def compute(part, _):
        load(part).wait()
        tensor, half, whole = place(part)

        def block(number, _):
            span = pl.ds(pl.multiple_of(number * block_rows, block_rows), block_rows)
            grads = grad_ref[tensor, half, pl.ds(pl.multiple_of(whole.start + number * block_rows, block_rows), block_rows)]
            values = adam_update(moved[part, 0, span], moved[part, 1, span], moved[part, 2, span], grads, clip_factor)
            for number, value in enumerate(values):
                results[part, number, span] = value
            return 0

        lax.fori_loop(0, rows // block_rows, block, 0)
        for copy in stores(part):
            copy.start()
        return 0

    def finish(part, _):
        for copy in stores(part):
            copy.wait()
        return 0

    lax.fori_loop(0, parts, begin, 0)
    lax.fori_loop(0, parts, compute, 0)
    lax.fori_loop(0, parts, finish, 0)


def update(table, clip_factor, moved, gradients):
    tensors, halves, rows, lanes = gradients.shape
    step = min(rows, PART)
    parts = tensors * halves * (rows // step)
    return pl.pallas_call(
        update_kernel,
        in_specs=[
            pl.BlockSpec(memory_space=pltpu.SMEM),
            pl.BlockSpec(memory_space=pltpu.VMEM),
            pl.BlockSpec(memory_space=pl.ANY),
            pl.BlockSpec(memory_space=pltpu.VMEM),
        ],
        out_specs=[pl.BlockSpec(memory_space=pl.ANY)] * 3,
        out_shape=[jax.ShapeDtypeStruct(gradients.shape, jnp.float32)] * 3,
        scratch_shapes=[
            pltpu.VMEM((parts, 3, step, lanes), jnp.float32),
            pltpu.VMEM((parts, 3, step, lanes), jnp.float32),
            pltpu.SemaphoreType.DMA((parts,)),
            pltpu.SemaphoreType.DMA((3, parts)),
        ],
        compiler_params=pltpu.CompilerParams(vmem_limit_bytes=20 << 20),
        name="update",
    )(table, clip_factor, moved, gradients)


def shards(old_params, old_first, old_second, gradients, old_table, new_table):
    tensors, halves, width = old_params.shape
    devices = lax.axis_size(AXES)
    rows = width // LANES
    old_key = old_table[:, 0]
    keys = jnp.bitwise_xor(jnp.right_shift(old_key, 1), new_table[:, 0])
    table = jnp.stack([jnp.bitwise_and(keys, 1), jnp.bitwise_and(old_key, 1)])
    chip_keys = jnp.right_shift(keys, 1)

    def paired(array):
        return array.reshape(tensors, halves, rows, 1, LANES).transpose(0, 2, 1, 3, 4)

    flat = gradients.reshape(tensors, halves, rows, LANES)
    clip_factor = clip_of(gradients, devices, 0)
    chip_keys, clip_factor = lax.optimization_barrier((chip_keys, clip_factor))
    chips = devices // 2
    states = (paired(old_params), paired(old_first), paired(old_second))
    if devices <= JOINT_DEVICES:

        def inner(one, arrays):
            branches = [
                functools.partial(move, ((0, 2 * one), (1, 2 * two)), 1 + one * chips + two) for two in range(chips)
            ]
            return lax.switch(chip_keys[1], branches, arrays)

        moved = lax.switch(chip_keys[0], [functools.partial(inner, one) for one in range(chips)], states)
    else:
        moved = []
        for tensor in range(tensors):
            branches = [
                functools.partial(move, ((tensor, 2 * i),), 1 + tensor * chips + i) for i in range(chips)
            ]
            moved.append(lax.switch(chip_keys[tensor], branches, states))
        moved = jnp.concatenate(moved, axis=1)
    results = update(table, clip_factor, moved, flat)
    return tuple(result.reshape(gradients.shape) for result in results)


def solution(mesh):
    spec = P(None, AXES, None)
    return jax.shard_map(
        shards,
        mesh=mesh,
        in_specs=(spec, spec, spec, spec, P(), P()),
        out_specs=(spec, spec, spec),
        check_vma=False,
    )
```

```python
import functools
import math

import jax
import jax.numpy as jnp
from jax import lax
from jax.experimental import pallas as pl
from jax.experimental.pallas import tpu as pltpu
from jax.sharding import PartitionSpec as P

STEP = 100
LANES = 128
AXES = ("row", "col")
JOINT_DEVICES = 32
GROUPS = 8
SPLIT = 2
PART = 1024
BLOCK = 256
SUM_ROWS = 256
LOGICAL = pl.DeviceIdType.LOGICAL


beta_one = 0.9
beta_two = 0.95
epsilon = 1e-08
learn_rate = 0.001
decay_rate = 0.1


def adam_update(params, first_moment, second_moment, gradients, clip_factor):
    scaled = clip_factor * gradients
    first_new = beta_one * first_moment + (1.0 - beta_one) * scaled
    second_new = beta_two * second_moment + (1.0 - beta_two) * scaled * scaled
    rate = learn_rate / (1.0 - beta_one**STEP)
    unbias = 1.0 / (1.0 - beta_two**STEP)
    update = first_new * rate / (jnp.sqrt(second_new * unbias) + epsilon)
    params_new = params * (1.0 - learn_rate * decay_rate) - update
    return (params_new, first_new, second_new)


def partner(key):
    return jnp.bitwise_xor(lax.axis_index(AXES), key)


def clip_kernel(devices, limit, grad_ref, clip_ref, grads, parts, load_sems, sent_sem, landed_sem):
    step = grads.shape[1]
    loads = [
        pltpu.make_async_copy(grad_ref.at[pl.ds(number * step, step)], grads.at[number], load_sems.at[number])
        for number in range(grads.shape[0])
    ]
    for load in loads:
        load.start()
    barrier = pltpu.get_barrier_semaphore()

    def greet(step, _):
        pl.semaphore_signal(barrier, inc=1, device_id=partner(devices - step), device_id_type=LOGICAL)
        return 0

    lax.fori_loop(1, devices, greet, 0)
    rows = min(step, SUM_ROWS)
    squares = jnp.zeros((8, LANES), jnp.float32)
    for number, load in enumerate(loads):
        load.wait()

        def add(line, total, number=number):
            block = grads[number, pl.ds(pl.multiple_of(line * rows, rows), rows)]
            return total + jnp.sum((block * block).reshape(-1, 8, LANES), axis=0)

        squares = lax.fori_loop(0, step // rows, add, squares)
    parts[0] = jnp.sum(squares, axis=0, keepdims=True)
    pl.semaphore_wait(barrier, devices - 1)

    def send(step, _):
        key = devices - step
        pltpu.make_async_remote_copy(
            src_ref=parts.at[0],
            dst_ref=parts.at[key],
            send_sem=sent_sem,
            recv_sem=landed_sem,
            device_id=partner(key),
            device_id_type=LOGICAL,
        ).start()
        return 0

    lax.fori_loop(1, devices, send, 0)
    others = parts.at[pl.ds(1, devices - 1)]
    pltpu.make_async_copy(others, others, landed_sem).wait()
    pltpu.make_async_copy(others, others, sent_sem).wait()
    total = jnp.sum(jnp.sum(parts[...], axis=0), axis=1, keepdims=True)
    clip_ref[...] = jnp.broadcast_to(limit / jnp.maximum(jnp.sqrt(total), limit), clip_ref.shape)


def clip_of(gradients, devices, number):
    limit = 0.5 * math.sqrt(gradients.size * devices)
    loads = 2
    step = gradients.size // LANES // loads
    return pl.pallas_call(
        functools.partial(clip_kernel, devices, limit),
        in_specs=[pl.BlockSpec(memory_space=pl.ANY)],
        out_specs=pl.BlockSpec(memory_space=pltpu.VMEM),
        out_shape=jax.ShapeDtypeStruct((1, LANES), jnp.float32),
        scratch_shapes=[
            pltpu.VMEM((loads, step, LANES), jnp.float32),
            pltpu.VMEM((devices, 1, LANES), jnp.float32),
            pltpu.SemaphoreType.DMA((loads,)),
            pltpu.SemaphoreType.DMA,
            pltpu.SemaphoreType.DMA,
        ],
        compiler_params=pltpu.CompilerParams(collective_id=number, has_side_effects=True),
        name="clip",
    )(gradients.reshape(-1, LANES))


def move_kernel(jobs, params_ref, first_ref, second_ref, out_ref, landed_sems, sent_sem, passed_sem):
    states = (params_ref, first_ref, second_ref)
    moves = [(slot, tensor, key) for slot, (tensor, key) in enumerate(jobs) if key]
    stays = [(slot, tensor) for slot, (tensor, key) in enumerate(jobs) if not key]
    peers = sorted({1} | {key for _, _, key in moves})
    places = {key: partner(key) for key in peers}
    barrier = pltpu.get_barrier_semaphore()
    for place in places.values():
        pl.semaphore_signal(barrier, inc=1, device_id=place, device_id_type=LOGICAL)
    pl.semaphore_wait(barrier, len(peers))
    (groups,) = landed_sems.shape
    halves = params_ref.shape[2]
    group_rows = params_ref.shape[1] // groups
    rows = max(group_rows // SPLIT, 1)
    split = group_rows // rows

    def span(start, size):
        return pl.ds(pl.multiple_of(start * size, size), size)

    def turn(step):
        (slot, tensor, key), (_, _, other) = moves[0], moves[-1]
        if len(moves) == 1:
            return slot, tensor, places[key], step
        bit = jnp.bitwise_and(step, 1)
        place = places[key]
        if key != other:
            place = jnp.where(bit == 0, place, places[other])
        return bit, bit, place, jnp.right_shift(step, 1)

    def window(slot, tensor, piece):
        half, chunk = jnp.bitwise_and(piece, 1), jnp.right_shift(piece, 1)
        for number, state in enumerate(states):
            source = state.at[tensor, span(chunk, rows), half, 0]
            yield source, out_ref.at[0, slot, number, half, span(chunk, rows)], landed_sems.at[lax.div(chunk, split)]

    def start(step, _):
        slot, tensor, place, piece = turn(step)
        for source, target, landed_sem in window(slot, tensor, piece):
            pltpu.make_async_remote_copy(
                src_ref=source,
                dst_ref=target,
                send_sem=sent_sem,
                recv_sem=landed_sem,
                device_id=place,
                device_id_type=LOGICAL,
            ).start()
        return 0

    def keep(step, _):
        slot, tensor, piece = stays[0] + (step,)
        if len(stays) == 2:
            slot, piece = jnp.bitwise_and(step, 1), jnp.right_shift(step, 1)
            tensor = slot
        for source, target, landed_sem in window(slot, tensor, piece):
            pltpu.make_async_copy(source, target, landed_sem).start()
        return 0

    def relay(group, _):
        landed = out_ref.at[0, :, :, :, span(group, group_rows)]
        pltpu.make_async_copy(landed, landed, landed_sems.at[group]).wait()
        pltpu.make_async_remote_copy(
            src_ref=landed,
            dst_ref=out_ref.at[1, :, :, :, span(group, group_rows)],
            send_sem=sent_sem,
            recv_sem=passed_sem,
            device_id=places[1],
            device_id_type=LOGICAL,
        ).start()
        return 0

    pieces = groups * split * halves
    if moves:
        lax.fori_loop(0, pieces * len(moves), start, 0)
    if stays:
        lax.fori_loop(0, pieces * len(stays), keep, 0)
    lax.fori_loop(0, groups, relay, 0)
    passed = out_ref.at[1]
    sent = passed if stays else out_ref
    pltpu.make_async_copy(sent, sent, sent_sem).wait()
    if moves and stays:
        moved = out_ref.at[0, moves[0][0]]
        pltpu.make_async_copy(moved, moved, sent_sem).wait()
    pltpu.make_async_copy(passed, passed, passed_sem).wait()


def move(jobs, number, arrays):
    _, rows, halves, _, lanes = arrays[0].shape
    groups = min(GROUPS, rows)
    return pl.pallas_call(
        functools.partial(move_kernel, jobs),
        in_specs=[pl.BlockSpec(memory_space=pl.ANY)] * 3,
        out_specs=pl.BlockSpec(memory_space=pl.ANY),
        out_shape=jax.ShapeDtypeStruct((2, len(jobs), 3, halves, rows, lanes), jnp.float32),
        scratch_shapes=[pltpu.SemaphoreType.DMA((groups,))] + [pltpu.SemaphoreType.DMA] * 2,
        compiler_params=pltpu.CompilerParams(
            collective_id=number, has_side_effects=True, vmem_limit_bytes=1 << 20
        ),
        name="move_" + "_".join(str(key) for _, key in jobs),
    )(*arrays)


def update_kernel(table_ref, clip_ref, moved_ref, grad_ref, params_out, first_out, second_out, *scratch):
    moved, results, moved_sems, out_sems = scratch
    parts, _, rows, _ = moved.shape
    halves = grad_ref.shape[1]
    blocks = grad_ref.shape[2] // rows
    block_rows = min(rows, BLOCK)
    outs = (params_out, first_out, second_out)
    clip_factor = clip_ref[...]

    def place(part):
        block, shard = lax.rem(part, blocks), lax.div(part, blocks)
        return lax.div(shard, halves), lax.rem(shard, halves), pl.ds(pl.multiple_of(block * rows, rows), rows)

    def load(part):
        tensor, half, span = place(part)
        source = moved_ref.at[table_ref[0, tensor], tensor, :, jnp.bitwise_xor(half, table_ref[1, tensor]), span]
        return pltpu.make_async_copy(source, moved.at[part], moved_sems.at[part])

    def stores(part):
        tensor, half, span = place(part)
        return [
            pltpu.make_async_copy(results.at[part, number], out.at[tensor, half, span], out_sems.at[number, part])
            for number, out in enumerate(outs)
        ]

    def begin(part, _):
        load(part).start()
        return 0

    def compute(part, _):
        load(part).wait()
        tensor, half, whole = place(part)

        def block(number, _):
            span = pl.ds(pl.multiple_of(number * block_rows, block_rows), block_rows)
            grads = grad_ref[tensor, half, pl.ds(pl.multiple_of(whole.start + number * block_rows, block_rows), block_rows)]
            values = adam_update(moved[part, 0, span], moved[part, 1, span], moved[part, 2, span], grads, clip_factor)
            for number, value in enumerate(values):
                results[part, number, span] = value
            return 0

        lax.fori_loop(0, rows // block_rows, block, 0)
        for copy in stores(part):
            copy.start()
        return 0

    def finish(part, _):
        for copy in stores(part):
            copy.wait()
        return 0

    lax.fori_loop(0, parts, begin, 0)
    lax.fori_loop(0, parts, compute, 0)
    lax.fori_loop(0, parts, finish, 0)


def update(table, clip_factor, moved, gradients):
    tensors, halves, rows, lanes = gradients.shape
    step = min(rows, PART)
    parts = tensors * halves * (rows // step)
    return pl.pallas_call(
        update_kernel,
        in_specs=[
            pl.BlockSpec(memory_space=pltpu.SMEM),
            pl.BlockSpec(memory_space=pltpu.VMEM),
            pl.BlockSpec(memory_space=pl.ANY),
            pl.BlockSpec(memory_space=pltpu.VMEM),
        ],
        out_specs=[pl.BlockSpec(memory_space=pl.ANY)] * 3,
        out_shape=[jax.ShapeDtypeStruct(gradients.shape, jnp.float32)] * 3,
        scratch_shapes=[
            pltpu.VMEM((parts, 3, step, lanes), jnp.float32),
            pltpu.VMEM((parts, 3, step, lanes), jnp.float32),
            pltpu.SemaphoreType.DMA((parts,)),
            pltpu.SemaphoreType.DMA((3, parts)),
        ],
        compiler_params=pltpu.CompilerParams(vmem_limit_bytes=20 << 20),
        name="update",
    )(table, clip_factor, moved, gradients)


def shards(old_params, old_first, old_second, gradients, old_table, new_table):
    tensors, halves, width = old_params.shape
    devices = lax.axis_size(AXES)
    rows = width // LANES
    old_key = old_table[:, 0]
    keys = jnp.bitwise_xor(jnp.right_shift(old_key, 1), new_table[:, 0])
    table = jnp.stack([jnp.bitwise_and(keys, 1), jnp.bitwise_and(old_key, 1)])
    chip_keys = jnp.right_shift(keys, 1)

    def paired(array):
        return array.reshape(tensors, halves, rows, 1, LANES).transpose(0, 2, 1, 3, 4)

    flat = gradients.reshape(tensors, halves, rows, LANES)
    clip_factor = clip_of(gradients, devices, 0)
    chip_keys, clip_factor = lax.optimization_barrier((chip_keys, clip_factor))
    chips = devices // 2
    states = (paired(old_params), paired(old_first), paired(old_second))
    if devices <= JOINT_DEVICES:

        def inner(one, arrays):
            branches = [
                functools.partial(move, ((0, 2 * one), (1, 2 * two)), 1 + one * chips + two) for two in range(chips)
            ]
            return lax.switch(chip_keys[1], branches, arrays)

        moved = lax.switch(chip_keys[0], [functools.partial(inner, one) for one in range(chips)], states)
    else:
        moved = []
        for tensor in range(tensors):
            branches = [
                functools.partial(move, ((tensor, 2 * i),), 1 + tensor * chips + i) for i in range(chips)
            ]
            moved.append(lax.switch(chip_keys[tensor], branches, states))
        moved = jnp.concatenate(moved, axis=1)
    results = update(table, clip_factor, moved, flat)
    return tuple(result.reshape(gradients.shape) for result in results)


def solution(mesh):
    spec = P(None, AXES, None)
    return jax.shard_map(
        shards,
        mesh=mesh,
        in_specs=(spec, spec, spec, spec, P(), P()),
        out_specs=(spec, spec, spec),
        check_vma=False,
    )
```

```python
import functools
import math

import jax
import jax.numpy as jnp
from jax import lax
from jax.experimental import pallas as pl
from jax.experimental.pallas import tpu as pltpu
from jax.sharding import PartitionSpec as P

STEP = 100
LANES = 128
AXES = ("row", "col")
JOINT_DEVICES = 32
GROUPS = 8
SPLIT = 2
PART = 1024
BLOCK = 128
SUM_ROWS = 128
LOGICAL = pl.DeviceIdType.LOGICAL


beta_one = 0.9
beta_two = 0.95
epsilon = 1e-08
learn_rate = 0.001
decay_rate = 0.1


def adam_update(params, first_moment, second_moment, gradients, clip_factor):
    scaled = clip_factor * gradients
    first_new = beta_one * first_moment + (1.0 - beta_one) * scaled
    second_new = beta_two * second_moment + (1.0 - beta_two) * scaled * scaled
    rate = learn_rate / (1.0 - beta_one**STEP)
    unbias = 1.0 / (1.0 - beta_two**STEP)
    update = first_new * rate / (jnp.sqrt(second_new * unbias) + epsilon)
    params_new = params * (1.0 - learn_rate * decay_rate) - update
    return (params_new, first_new, second_new)


def partner(key):
    return jnp.bitwise_xor(lax.axis_index(AXES), key)


def clip_kernel(devices, limit, grad_ref, clip_ref, grads, parts, load_sems, sent_sem, landed_sem):
    step = grads.shape[1]
    loads = [
        pltpu.make_async_copy(grad_ref.at[pl.ds(number * step, step)], grads.at[number], load_sems.at[number])
        for number in range(grads.shape[0])
    ]
    for load in loads:
        load.start()
    barrier = pltpu.get_barrier_semaphore()

    def greet(step, _):
        pl.semaphore_signal(barrier, inc=1, device_id=partner(devices - step), device_id_type=LOGICAL)
        return 0

    lax.fori_loop(1, devices, greet, 0)
    rows = min(step, SUM_ROWS)
    squares = jnp.zeros((8, LANES), jnp.float32)
    for number, load in enumerate(loads):
        load.wait()

        def add(line, total, number=number):
            block = grads[number, pl.ds(pl.multiple_of(line * rows, rows), rows)]
            return total + jnp.sum((block * block).reshape(-1, 8, LANES), axis=0)

        squares = lax.fori_loop(0, step // rows, add, squares)
    parts[0] = jnp.sum(squares, axis=0, keepdims=True)
    pl.semaphore_wait(barrier, devices - 1)

    def send(step, _):
        key = devices - step
        pltpu.make_async_remote_copy(
            src_ref=parts.at[0],
            dst_ref=parts.at[key],
            send_sem=sent_sem,
            recv_sem=landed_sem,
            device_id=partner(key),
            device_id_type=LOGICAL,
        ).start()
        return 0

    lax.fori_loop(1, devices, send, 0)
    others = parts.at[pl.ds(1, devices - 1)]
    pltpu.make_async_copy(others, others, landed_sem).wait()
    pltpu.make_async_copy(others, others, sent_sem).wait()
    total = jnp.sum(jnp.sum(parts[...], axis=0), axis=1, keepdims=True)
    clip_ref[...] = jnp.broadcast_to(limit / jnp.maximum(jnp.sqrt(total), limit), clip_ref.shape)


def clip_of(gradients, devices, number):
    limit = 0.5 * math.sqrt(gradients.size * devices)
    loads = 2
    step = gradients.size // LANES // loads
    return pl.pallas_call(
        functools.partial(clip_kernel, devices, limit),
        in_specs=[pl.BlockSpec(memory_space=pl.ANY)],
        out_specs=pl.BlockSpec(memory_space=pltpu.VMEM),
        out_shape=jax.ShapeDtypeStruct((1, LANES), jnp.float32),
        scratch_shapes=[
            pltpu.VMEM((loads, step, LANES), jnp.float32),
            pltpu.VMEM((devices, 1, LANES), jnp.float32),
            pltpu.SemaphoreType.DMA((loads,)),
            pltpu.SemaphoreType.DMA,
            pltpu.SemaphoreType.DMA,
        ],
        compiler_params=pltpu.CompilerParams(collective_id=number, has_side_effects=True),
        name="clip",
    )(gradients.reshape(-1, LANES))


def move_kernel(jobs, params_ref, first_ref, second_ref, out_ref, landed_sems, sent_sem, passed_sem):
    states = (params_ref, first_ref, second_ref)
    moves = [(slot, tensor, key) for slot, (tensor, key) in enumerate(jobs) if key]
    stays = [(slot, tensor) for slot, (tensor, key) in enumerate(jobs) if not key]
    peers = sorted({1} | {key for _, _, key in moves})
    places = {key: partner(key) for key in peers}
    barrier = pltpu.get_barrier_semaphore()
    for place in places.values():
        pl.semaphore_signal(barrier, inc=1, device_id=place, device_id_type=LOGICAL)
    pl.semaphore_wait(barrier, len(peers))
    (groups,) = landed_sems.shape
    halves = params_ref.shape[2]
    group_rows = params_ref.shape[1] // groups
    split = SPLIT if group_rows % SPLIT == 0 else 1
    rows = group_rows // split

    def span(start, size):
        return pl.ds(pl.multiple_of(start * size, size), size)

    def turn(step):
        (slot, tensor, key), (_, _, other) = moves[0], moves[-1]
        if len(moves) == 1:
            return slot, tensor, places[key], step
        bit = jnp.bitwise_and(step, 1)
        place = places[key]
        if key != other:
            place = jnp.where(bit == 0, place, places[other])
        return bit, bit, place, jnp.right_shift(step, 1)

    def across(source, target):
        return pltpu.make_async_remote_copy(
            src_ref=source,
            dst_ref=target,
            send_sem=sent_sem,
            recv_sem=passed_sem,
            device_id=places[1],
            device_id_type=LOGICAL,
        )

    def window(copy, slot, tensor, piece):
        half, chunk = jnp.bitwise_and(piece, 1), jnp.right_shift(piece, 1)
        for number, state in enumerate(states):
            source = state.at[tensor, span(chunk, rows), half, 0]
            yield source, out_ref.at[copy, slot, number, half, span(chunk, rows)], landed_sems.at[jnp.right_shift(chunk, split.bit_length() - 1)]

    def start(step, _):
        slot, tensor, place, piece = turn(step)
        for source, target, landed_sem in window(0, slot, tensor, piece):
            pltpu.make_async_remote_copy(
                src_ref=source,
                dst_ref=target,
                send_sem=sent_sem,
                recv_sem=landed_sem,
                device_id=place,
                device_id_type=LOGICAL,
            ).start()
        return 0

    def offer(step, _):
        slot, tensor, piece = stays[0] + (step,)
        if len(stays) == 2:
            slot, piece = jnp.bitwise_and(step, 1), jnp.right_shift(step, 1)
            tensor = slot
        for source, target, _ in window(1, slot, tensor, piece):
            across(source, target).start()
        return 0

    def relay(group, _):
        slots = moves[0][0] if stays else slice(None)
        landed = out_ref.at[0, slots, :, :, span(group, group_rows)]
        pltpu.make_async_copy(landed, landed, landed_sems.at[group]).wait()
        across(landed, out_ref.at[1, slots, :, :, span(group, group_rows)]).start()
        return 0

    pieces = groups * split * halves
    if moves:
        lax.fori_loop(0, pieces * len(moves), start, 0)
    if stays:
        lax.fori_loop(0, pieces * len(stays), offer, 0)
    if moves:
        lax.fori_loop(0, groups, relay, 0)
    passed = out_ref.at[1]
    sent = passed if stays else out_ref
    pltpu.make_async_copy(sent, sent, sent_sem).wait()
    if moves and stays:
        moved = out_ref.at[0, moves[0][0]]
        pltpu.make_async_copy(moved, moved, sent_sem).wait()
    pltpu.make_async_copy(passed, passed, passed_sem).wait()


def move(jobs, number, arrays):
    _, rows, halves, _, lanes = arrays[0].shape
    groups = min(GROUPS, rows)
    return pl.pallas_call(
        functools.partial(move_kernel, jobs),
        in_specs=[pl.BlockSpec(memory_space=pl.ANY)] * 3,
        out_specs=pl.BlockSpec(memory_space=pl.ANY),
        out_shape=jax.ShapeDtypeStruct((2, len(jobs), 3, halves, rows, lanes), jnp.float32),
        scratch_shapes=[pltpu.SemaphoreType.DMA((groups,))] + [pltpu.SemaphoreType.DMA] * 2,
        compiler_params=pltpu.CompilerParams(
            collective_id=number, has_side_effects=True, vmem_limit_bytes=1 << 20
        ),
        name="move_" + "_".join(str(key) for _, key in jobs),
    )(*arrays)


def update_kernel(table_ref, clip_ref, moved_ref, grad_ref, *rest):
    states, (params_out, first_out, second_out), scratch = rest[:3], rest[3:6], rest[6:]
    moved, results, moved_sems, out_sems = scratch
    parts, _, rows, _ = moved.shape
    halves = grad_ref.shape[1]
    blocks = grad_ref.shape[2] // rows
    block_rows = min(rows, BLOCK)
    outs = (params_out, first_out, second_out)
    clip_factor = clip_ref[...]

    def place(part):
        block, shard = lax.rem(part, blocks), lax.div(part, blocks)
        return lax.div(shard, halves), lax.rem(shard, halves), pl.ds(pl.multiple_of(block * rows, rows), rows)

    def load(part):
        tensor, half, span = place(part)
        source = moved_ref.at[table_ref[0, tensor], tensor, :, jnp.bitwise_xor(half, table_ref[1, tensor]), span]
        return pltpu.make_async_copy(source, moved.at[part], moved_sems.at[part])

    def begin(part, _):
        tensor, half, span = place(part)
        stays = table_ref[2, tensor] == 0

        @pl.when(jnp.logical_not(stays))
        def _():
            load(part).start()

        @pl.when(stays)
        def _():
            for number, state in enumerate(states):
                source = state.at[tensor, span, jnp.bitwise_xor(half, table_ref[1, tensor]), 0]
                pltpu.make_async_copy(source, moved.at[part, number], moved_sems.at[part]).start()

        return 0

    def stores(part):
        tensor, half, span = place(part)
        return [
            pltpu.make_async_copy(results.at[part, number], out.at[tensor, half, span], out_sems.at[number, part])
            for number, out in enumerate(outs)
        ]

    def compute(part, _):
        load(part).wait()
        tensor, half, whole = place(part)

        def block(number, _):
            span = pl.ds(pl.multiple_of(number * block_rows, block_rows), block_rows)
            grads = grad_ref[tensor, half, pl.ds(pl.multiple_of(whole.start + number * block_rows, block_rows), block_rows)]
            values = adam_update(moved[part, 0, span], moved[part, 1, span], moved[part, 2, span], grads, clip_factor)
            for number, value in enumerate(values):
                results[part, number, span] = value
            return 0

        lax.fori_loop(0, rows // block_rows, block, 0)
        for copy in stores(part):
            copy.start()
        return 0

    def finish(part, _):
        for copy in stores(part):
            copy.wait()
        return 0

    lax.fori_loop(0, parts, begin, 0)
    lax.fori_loop(0, parts, compute, 0)
    lax.fori_loop(0, parts, finish, 0)


def update(table, clip_factor, moved, gradients, states):
    tensors, halves, rows, lanes = gradients.shape
    step = min(rows, PART)
    parts = tensors * halves * (rows // step)
    return pl.pallas_call(
        update_kernel,
        in_specs=[
            pl.BlockSpec(memory_space=pltpu.SMEM),
            pl.BlockSpec(memory_space=pltpu.VMEM),
            pl.BlockSpec(memory_space=pl.ANY),
            pl.BlockSpec(memory_space=pltpu.VMEM),
        ]
        + [pl.BlockSpec(memory_space=pl.ANY)] * 3,
        out_specs=[pl.BlockSpec(memory_space=pl.ANY)] * 3,
        out_shape=[jax.ShapeDtypeStruct(gradients.shape, jnp.float32)] * 3,
        scratch_shapes=[
            pltpu.VMEM((parts, 3, step, lanes), jnp.float32),
            pltpu.VMEM((parts, 3, step, lanes), jnp.float32),
            pltpu.SemaphoreType.DMA((parts,)),
            pltpu.SemaphoreType.DMA((3, parts)),
        ],
        compiler_params=pltpu.CompilerParams(vmem_limit_bytes=20 << 20),
        name="update",
    )(table, clip_factor, moved, gradients, *states)


def shards(old_params, old_first, old_second, gradients, old_table, new_table):
    tensors, halves, width = old_params.shape
    devices = lax.axis_size(AXES)
    rows = width // LANES
    old_key = old_table[:, 0]
    keys = jnp.bitwise_xor(jnp.right_shift(old_key, 1), new_table[:, 0])
    table = jnp.stack([jnp.bitwise_and(keys, 1), jnp.bitwise_and(old_key, 1), keys])
    chip_keys = jnp.right_shift(keys, 1)

    def paired(array):
        return array.reshape(tensors, halves, rows, 1, LANES).transpose(0, 2, 1, 3, 4)

    flat = gradients.reshape(tensors, halves, rows, LANES)
    clip_factor = clip_of(gradients, devices, 0)
    chip_keys, clip_factor = lax.optimization_barrier((chip_keys, clip_factor))
    chips = devices // 2
    states = (paired(old_params), paired(old_first), paired(old_second))
    if devices <= JOINT_DEVICES:

        def inner(one, arrays):
            branches = [
                functools.partial(move, ((0, 2 * one), (1, 2 * two)), 1 + one * chips + two) for two in range(chips)
            ]
            return lax.switch(chip_keys[1], branches, arrays)

        moved = lax.switch(chip_keys[0], [functools.partial(inner, one) for one in range(chips)], states)
    else:
        moved = []
        for tensor in range(tensors):
            branches = [
                functools.partial(move, ((tensor, 2 * i),), 1 + tensor * chips + i) for i in range(chips)
            ]
            moved.append(lax.switch(chip_keys[tensor], branches, states))
        moved = jnp.concatenate(moved, axis=1)
    results = update(table, clip_factor, moved, flat, states)
    return tuple(result.reshape(gradients.shape) for result in results)


def solution(mesh):
    spec = P(None, AXES, None)
    return jax.shard_map(
        shards,
        mesh=mesh,
        in_specs=(spec, spec, spec, spec, P(), P()),
        out_specs=(spec, spec, spec),
        check_vma=False,
    )
```
